32 devices in a mesh: grp: 4 (over y, x), dev: 8 (over z, core).
Axes of the slice: x: 2, y: 2, z: 4, core: 2. Of those that a mesh axis runs over, the one named last changes fastest.
Arguments:
- source_id: int32 [524288], P(('grp', 'dev')), may hold values from 0 to 4095, as said below
- slot: int32 [524288], P(('grp', 'dev')), may hold values from 0 to 127, as said below
- owner: int32 [4096], replicated, may hold values from 0 to 4095, as said below
- counts: int32 [4096], P(('grp', 'dev')), may hold values from 1 to 128, as said below
- partials: float32 [5, 524288], P(None, ('grp', 'dev')), may hold values from -6 to 6
- residual: float32 [524288], P(('grp', 'dev')), may hold values from -6 to 6
- weight: float32 [524288], P(('grp', 'dev')), may hold values from 0.3 to 9
- prior: float32 [5, 4096], P(None, ('grp', 'dev')), may hold values from 0.5 to 4
Outputs:
- updates: float32 [5, 4096], P(None, ('grp', 'dev'))
- standardized: float32 [524288], P(('grp', 'dev'))
- norm: float32 [], replicated
The draws below stay inside these ranges and needn't reach their ends.
Inputs may be any that keep to these rules, and one draw needn't show every extreme that they name: A permutation: source s stands at owner position owner[s], and position p belongs to device p // 128. `source_id`: the rows of one device stand in 32 aligned blocks of 512 rows; block k holds only rows whose source's owner position lies in device k's range. Over all rows, each pair of a source and a slot below 128 appears exactly once. A row is an observation when its slot is below its source's count, else padding. Each device's block of counts holds 128 at least once.
All inputs are finite; a program needn't handle non-finite values.
Results may differ from the reference program's by a relative error of at most 0.0003.
Values sent between devices are 32-bit elements; how exact they have to be, the bound alone decides.
A program may use at most 64 MiB of HBM per device.

```python
import math
import jax
import jax.numpy as jnp
from jax import lax

PARAMS = 5
PAD = 128
SRC_DEV = 128
SOURCES = 4096
ROWS_DEV = 16384
ROWS_ALL = 524288
CAP = 512
N_GRP = 4
N_DEV = 8


def row_layout(key):
    base_key = jax.random.fold_in(key, 7001)
    devices_all = N_GRP * N_DEV
    placing = jax.random.permutation(jax.random.fold_in(base_key, 1), SOURCES).astype(jnp.int32)
    at_position = jnp.argsort(placing, stable=True).astype(jnp.int32)

    def owner_cells(owner_k):
        return jax.random.permutation(jax.random.fold_in(base_key, 1000 + owner_k), ROWS_DEV).astype(jnp.int32)
    cell_map = jax.vmap(owner_cells)(jnp.arange(devices_all, dtype=jnp.int32))
    cell_map = cell_map.reshape(devices_all, devices_all, CAP).transpose(1, 0, 2)
    owner_of = jnp.broadcast_to(jnp.arange(devices_all, dtype=jnp.int32)[None, :, None], cell_map.shape)
    position = owner_of * SRC_DEV + cell_map // PAD
    source_ids = at_position[position.reshape(-1)]
    slots = (cell_map % PAD).reshape(-1)
    return (placing, source_ids, slots)


def draw_owner(key, part):
    return row_layout(key)[0]


def draw_source_id(key, part):
    return row_layout(key)[1]


def draw_slot(key, part):
    return row_layout(key)[2]


def draw_counts(key, part):
    base_key = jax.random.fold_in(key, 7002)
    first_try = jax.random.randint(jax.random.fold_in(base_key, 1), (SOURCES,), 1, PAD + 1)
    second_try = jax.random.randint(jax.random.fold_in(base_key, 2), (SOURCES,), 1, PAD + 1)
    few_obs = jax.random.randint(jax.random.fold_in(base_key, 3), (SOURCES,), 1, PAD // 8 + 1)
    pick_low = jax.random.randint(jax.random.fold_in(base_key, 4), (SOURCES,), 0, 4) == 0
    result = jnp.where(pick_low, few_obs, jnp.maximum(first_try, second_try))
    full_slot = jax.random.randint(jax.random.fold_in(base_key, 5), (N_GRP * N_DEV,), 0, SRC_DEV)
    spots = jnp.arange(SOURCES, dtype=jnp.int32)
    result = jnp.where(spots % SRC_DEV == full_slot[spots // SRC_DEV], PAD, result)
    return result.astype(jnp.int32)


def draw_weight(key, part):
    row_device = jnp.arange(ROWS_ALL, dtype=jnp.int32) // ROWS_DEV
    rising = 1.0 + 2.0 * row_device.astype(jnp.float32) / max(N_GRP * N_DEV - 1, 1)
    spread = jnp.exp(jax.random.uniform(key, (ROWS_ALL,), jnp.float32, math.log(0.3), math.log(3.0)))
    return (spread * rising).astype(jnp.float32)


def steps_of(stream_key, shape, cuts, smallest, high):
    level, own = 1.0, jax.random.fold_in(stream_key, 6)
    for dim, blocks in cuts:
        heights = jnp.exp(jax.random.uniform(jax.random.fold_in(own, dim), (blocks,), jnp.float32, smallest / len(cuts), high / len(cuts)))
        level = level * jnp.repeat(heights, shape[dim] // blocks).reshape([-1 if axis == dim else 1 for axis in range(len(shape))])
    return level


def gaussian(own_key, extent, width, bound, pieces=(), kind=jnp.bfloat16):
    factor_of = steps_of(own_key, extent, pieces, -0.22, 0.18) if pieces else 1.0
    values = jax.random.normal(own_key, extent, jnp.float32) * width * factor_of
    return jnp.minimum(jnp.maximum(values, -bound), bound).astype(kind)


def setup_inputs(seed: int = 0) -> dict:
    streams_of = jax.random.split(jax.random.key(seed), 9)
    source_id = draw_source_id(jax.random.fold_in(streams_of[8], 71), 0)
    slot = draw_slot(jax.random.fold_in(streams_of[8], 71), 0)
    owner = draw_owner(jax.random.fold_in(streams_of[8], 71), 0)
    counts = draw_counts(jax.random.fold_in(streams_of[8], 71), 0)
    partials = gaussian(streams_of[4], (PARAMS, ROWS_ALL), 1.0, 6.0, ((1, 32),), jnp.float32)
    residual = gaussian(streams_of[5], (ROWS_ALL,), 1.0, 6.0, ((0, 32),), jnp.float32)
    weight = draw_weight(jax.random.fold_in(streams_of[8], 71), 0)
    prior = jnp.clip(jnp.exp(math.log(4.0) - 2.0794415 * jax.random.uniform(streams_of[7], (PARAMS, SOURCES), jnp.float32) ** steps_of(streams_of[7], (PARAMS, SOURCES), ((1, 32),), -0.2, 0.2)), 0.5, 4.0)
    return dict(source_id=source_id, slot=slot, owner=owner, counts=counts, partials=partials, residual=residual, weight=weight, prior=prior)


def solve_blocks(normal, moments):
    params = len(moments)
    factor = {}
    for column in range(params):
        running = normal[column][column]
        for earlier in range(column):
            running = running - factor[column, earlier] ** 2
        pivot_value = jnp.sqrt(running)
        factor[column, column] = pivot_value
        for target in range(column + 1, params):
            current = normal[target][column]
            for earlier in range(column):
                current = current - factor[target, earlier] * factor[column, earlier]
            factor[target, column] = current / pivot_value
    forward = []
    for target in range(params):
        current = moments[target]
        for earlier in range(target):
            current = current - factor[target, earlier] * forward[earlier]
        forward.append(current / factor[target, target])
    backward = [None] * params
    for target in reversed(range(params)):
        current = forward[target]
        for later in range(target + 1, params):
            current = current - factor[later, target] * backward[later]
        backward[target] = current / factor[target, target]
    return jnp.stack(backward)

def reference(source_id, slot, owner, counts, partials, residual, weight, prior):
    params = partials.shape[0]
    position = owner[source_id]
    live_mask = (slot < counts[position]).astype(jnp.float32)
    weighted = partials * (weight * live_mask)[None, :]
    normal = [[None] * params for _ in range(params)]
    for first_idx in range(params):
        for second_idx in range(first_idx, params):
            entry = jax.ops.segment_sum(weighted[first_idx] * partials[second_idx], position, num_segments=SOURCES)
            if first_idx == second_idx:
                entry = entry + prior[first_idx]
            normal[first_idx][second_idx] = entry
            normal[second_idx][first_idx] = entry
    moments = [jax.ops.segment_sum(weighted[first_idx] * residual, position, num_segments=SOURCES) for first_idx in range(params)]
    updates = solve_blocks(normal, moments)
    fitted = lax.optimization_barrier(jnp.sum(partials * updates[:, position], axis=0))
    fresh = (residual - fitted) * live_mask
    squares = jnp.sum(weight * fresh * fresh)
    live_total = jnp.sum(live_mask)
    norm = jnp.sqrt(squares / live_total + 1e-06)
    return (updates, fresh * jnp.sqrt(weight) / norm, norm)
```

```python
import functools

import jax
import jax.numpy as jnp
from jax import lax
from jax.experimental import pallas as pl
from jax.experimental.pallas import tpu as pltpu
from jax.sharding import PartitionSpec as P

LANES = 128
SUBLANES = 8
MESH = pl.DeviceIdType.MESH


def solve_rows(normal, moments):
    params = len(moments)
    factor = {}
    for column in range(params):
        running = normal[column][column]
        for earlier in range(column):
            running = running - factor[column, earlier] ** 2
        pivot_value = jnp.sqrt(running)
        factor[column, column] = pivot_value
        for target in range(column + 1, params):
            current = normal[target][column]
            for earlier in range(column):
                current = current - factor[target, earlier] * factor[column, earlier]
            factor[target, column] = current / pivot_value
    forward = []
    for target in range(params):
        current = moments[target]
        for earlier in range(target):
            current = current - factor[target, earlier] * forward[earlier]
        forward.append(current / factor[target, target])
    backward = [None] * params
    for target in reversed(range(params)):
        current = forward[target]
        for later in range(target + 1, params):
            current = current - factor[later, target] * backward[later]
        backward[target] = current / factor[target, target]
    return backward


def thirds(values):
    high = values.astype(jnp.bfloat16).astype(jnp.float32)
    rest = values - high
    middle = rest.astype(jnp.bfloat16).astype(jnp.float32)
    return [high, middle, rest - middle]


def stacked(values, rows):
    terms = thirds(values)
    spare = rows - 3 * values.shape[0]
    if spare:
        terms.append(jnp.zeros((spare, values.shape[1]), jnp.float32))
    return jnp.concatenate(terms, axis=0).astype(jnp.bfloat16)


def kernel(
    sizes,
    source_ref, slot_ref, owner_ref, counts_ref, partials_ref, residual_ref, weight_ref, prior_ref,
    updates_ref, fresh_ref, norm_ref,
    out_buf, in_buf, hot_buf, back_out, back_in,
    send_sem, recv_sem, back_send_sem, back_recv_sem,
):
    n, members, width = sizes
    params = partials_ref.shape[0]
    src_local = counts_ref.shape[1]
    me = lax.axis_index("grp") * members + lax.axis_index("dev")

    def coords(device):
        return (device // members, device % members)

    barrier = pltpu.get_barrier_semaphore()

    def greet(step, carry):
        peer = (me + step) % n
        pl.semaphore_signal(barrier, inc=1, device_id=coords(peer), device_id_type=MESH)
        return carry

    lax.fori_loop(1, n, greet, 0)

    def prepare(k, carry):
        cols = pl.ds(pl.multiple_of(k * width, LANES), width)
        root = jnp.sqrt(weight_ref[:, cols])
        out_buf[k, 0:params, :] = partials_ref[:, cols] * root
        out_buf[k, params : params + 1, :] = residual_ref[:, cols] * root
        out_buf[k, params + 1 : params + 2, :] = source_ref[:, cols].astype(jnp.float32)
        out_buf[k, params + 2 : params + 3, :] = slot_ref[:, cols].astype(jnp.float32)
        return carry

    lax.fori_loop(0, n, prepare, 0)

    pl.semaphore_wait(barrier, n - 1)

    def send(step, carry):
        peer = (me + step) % n
        pltpu.make_async_remote_copy(
            src_ref=out_buf.at[peer],
            dst_ref=in_buf.at[me],
            send_sem=send_sem,
            recv_sem=recv_sem.at[me],
            device_id=coords(peer),
            device_id_type=MESH,
        ).start()
        return carry

    lax.fori_loop(1, n, send, 0)

    position = me * src_local + lax.broadcasted_iota(jnp.int32, (src_local, LANES), 0)

    def invert(tile, total):
        ids = tile * LANES + lax.broadcasted_iota(jnp.int32, (1, LANES), 1)
        return total + jnp.where(owner_ref[pl.ds(tile, 1), :] == position, ids, 0)

    found = lax.fori_loop(0, owner_ref.shape[0], invert, jnp.zeros((src_local, LANES), jnp.int32))
    source_at = jnp.sum(found.astype(jnp.float32), axis=1, keepdims=True)

    counts = counts_ref[...].astype(jnp.float32)
    count_table = jnp.broadcast_to(counts, (2 * SUBLANES, src_local)).astype(jnp.bfloat16)

    def absorb(k, total):
        rows = in_buf[k]
        hot = (rows[params + 1 : params + 2, :] == source_at).astype(jnp.float32).astype(jnp.bfloat16)
        hot_buf[k] = hot
        row_counts = jnp.dot(count_table, hot, preferred_element_type=jnp.float32)[0:SUBLANES]
        rows = jnp.where(rows[params + 2 : params + 3, :] < row_counts, rows, 0.0)
        in_buf[k] = rows
        products = jnp.concatenate([rows[i : i + 1, :] * rows for i in range(params)], axis=0)
        return total + lax.dot_general(
            stacked(products, LANES), hot, (((1,), (1,)), ((), ())), preferred_element_type=jnp.float32
        )

    in_buf[me] = out_buf[me]
    total = absorb(me, jnp.zeros((LANES, src_local), jnp.float32))

    def arrive(step, total):
        peer = (me + n - step) % n
        pltpu.make_async_remote_copy(
            src_ref=out_buf.at[peer],
            dst_ref=in_buf.at[peer],
            send_sem=send_sem,
            recv_sem=recv_sem.at[peer],
            device_id=coords(peer),
            device_id_type=MESH,
        ).wait_recv()
        return absorb(peer, total)

    total = lax.fori_loop(1, n, arrive, total)

    height = params * SUBLANES
    sums = total[0:height] + total[height : 2 * height] + total[2 * height : 3 * height]
    normal = [[None] * params for _ in range(params)]
    for i in range(params):
        for j in range(i, params):
            entry = sums[i * SUBLANES + j : i * SUBLANES + j + 1]
            if i == j:
                entry = entry + prior_ref[i : i + 1, :]
            normal[i][j] = entry
            normal[j][i] = entry
    moments = [sums[i * SUBLANES + params : i * SUBLANES + params + 1] for i in range(params)]
    updates = solve_rows(normal, moments)
    for i in range(params):
        updates_ref[i : i + 1, :] = updates[i]
    blank = jnp.zeros((1, src_local), jnp.float32)
    table = jnp.concatenate(updates + [blank - 1.0, blank, blank], axis=0)
    table = stacked(table, 4 * SUBLANES)

    def refit(k, squares):
        spread = jnp.dot(table, hot_buf[k], preferred_element_type=jnp.float32)
        spread = spread[0:SUBLANES] + spread[SUBLANES : 2 * SUBLANES] + spread[2 * SUBLANES : 3 * SUBLANES]
        fresh = -jnp.sum(in_buf[k] * spread, axis=0, keepdims=True)
        back_out[k, :, 0:width] = fresh
        return squares + fresh * fresh

    squares = lax.fori_loop(0, n, refit, jnp.zeros((1, width), jnp.float32))
    lane = lax.broadcasted_iota(jnp.int32, (1, LANES), 1)
    square_sum = jnp.sum(squares, axis=1, keepdims=True)
    count_sum = jnp.sum(counts, axis=1, keepdims=True)
    tail = jnp.where(lane == 0, square_sum, jnp.where(lane == 1, count_sum, 0.0))

    def finish(k, carry):
        back_out[k, :, width : width + LANES] = tail
        return carry

    lax.fori_loop(0, n, finish, 0)
    back_in[me] = back_out[me]

    def send_back(step, carry):
        peer = (me + step) % n
        pltpu.make_async_remote_copy(
            src_ref=back_out.at[peer],
            dst_ref=back_in.at[me],
            send_sem=back_send_sem,
            recv_sem=back_recv_sem.at[me],
            device_id=coords(peer),
            device_id_type=MESH,
        ).start()
        return carry

    lax.fori_loop(1, n, send_back, 0)

    def collect(step, tails):
        peer = (me + n - step) % n
        pltpu.make_async_remote_copy(
            src_ref=back_out.at[peer],
            dst_ref=back_in.at[peer],
            send_sem=back_send_sem,
            recv_sem=back_recv_sem.at[peer],
            device_id=coords(peer),
            device_id_type=MESH,
        ).wait_recv()
        return tails

    lax.fori_loop(1, n, collect, 0)

    def gather_tails(k, tails):
        return tails + back_in[k, :, width : width + LANES]

    tails = lax.fori_loop(0, n, gather_tails, jnp.zeros((1, LANES), jnp.float32))
    square_total = jnp.sum(jnp.where(lane == 0, tails, 0.0), axis=1, keepdims=True)
    count_total = jnp.sum(jnp.where(lane == 1, tails, 0.0), axis=1, keepdims=True)
    norm = jnp.sqrt(square_total / count_total + 1e-06)
    norm_ref[...] = jnp.broadcast_to(norm, norm_ref.shape)
    scale = 1.0 / norm

    def emit(k, carry):
        cols = pl.ds(pl.multiple_of(k * width, LANES), width)
        fresh_ref[:, cols] = back_in[k, :, 0:width] * scale
        return carry

    lax.fori_loop(0, n, emit, 0)

    for buffer, semaphore in ((out_buf, send_sem), (back_out, back_send_sem)):
        sent = buffer.at[pl.ds(0, n - 1)]
        pltpu.make_async_remote_copy(
            src_ref=sent,
            dst_ref=sent,
            send_sem=semaphore,
            recv_sem=recv_sem.at[me],
            device_id=coords((me + 1) % n),
            device_id_type=MESH,
        ).wait_send()


def body(source_id, slot, owner, counts, partials, residual, weight, prior):
    members = lax.axis_size("dev")
    n = lax.axis_size("grp") * members
    params = partials.shape[0]
    row_count = residual.shape[0]
    src_local = counts.shape[0]
    block_rows = row_count // n
    width = -(-block_rows // LANES) * LANES

    def lay(array, fill):
        array = array.reshape(-1, row_count)
        if width == block_rows:
            return array
        blocks = array.reshape(-1, n, block_rows)
        blocks = jnp.pad(blocks, ((0, 0), (0, 0), (0, width - block_rows)), constant_values=fill)
        return blocks.reshape(-1, n * width)

    vmem = pl.BlockSpec(memory_space=pltpu.VMEM)
    updates, standardized, norm = pl.pallas_call(
        functools.partial(kernel, (n, members, width)),
        out_shape=(
            jax.ShapeDtypeStruct((params, src_local), jnp.float32),
            jax.ShapeDtypeStruct((1, n * width), jnp.float32),
            jax.ShapeDtypeStruct((1, LANES), jnp.float32),
        ),
        in_specs=[vmem] * 8,
        out_specs=(vmem, vmem, vmem),
        scratch_shapes=[
            pltpu.VMEM((n, SUBLANES, width), jnp.float32),
            pltpu.VMEM((n, SUBLANES, width), jnp.float32),
            pltpu.VMEM((n, src_local, width), jnp.bfloat16),
            pltpu.VMEM((n, 1, width + LANES), jnp.float32),
            pltpu.VMEM((n, 1, width + LANES), jnp.float32),
            pltpu.SemaphoreType.DMA,
            pltpu.SemaphoreType.DMA((n,)),
            pltpu.SemaphoreType.DMA,
            pltpu.SemaphoreType.DMA((n,)),
        ],
        compiler_params=pltpu.CompilerParams(
            collective_id=0, has_side_effects=True, vmem_limit_bytes=48 * 1024 * 1024
        ),
        name="exchange_fit",
    )(
        lay(source_id, -1),
        lay(slot, 0),
        owner.reshape(-1, LANES),
        counts.reshape(1, src_local),
        lay(partials, 0),
        lay(residual, 0),
        lay(weight, 1),
        prior,
    )
    standardized = standardized.reshape(n, width)[:, :block_rows] if width != block_rows else standardized
    return (updates, standardized.reshape(row_count), norm[0, 0])


def solution(mesh):
    in_specs = (
        P(("grp", "dev")),
        P(("grp", "dev")),
        P(),
        P(("grp", "dev")),
        P(None, ("grp", "dev")),
        P(("grp", "dev")),
        P(("grp", "dev")),
        P(None, ("grp", "dev")),
    )
    out_specs = (P(None, ("grp", "dev")), P(("grp", "dev")), P())
    return jax.shard_map(body, mesh=mesh, in_specs=in_specs, out_specs=out_specs, check_vma=False)
```

```python
import functools

import jax
import jax.numpy as jnp
from jax import lax
from jax.experimental import pallas as pl
from jax.experimental.pallas import tpu as pltpu
from jax.sharding import PartitionSpec as P

LANES = 128
SUBLANES = 8
UNROLL = 4
MESH = pl.DeviceIdType.MESH


def solve_rows(normal, moments):
    params = len(moments)
    factor = {}
    for column in range(params):
        running = normal[column][column]
        for earlier in range(column):
            running = running - factor[column, earlier] ** 2
        pivot_value = jnp.sqrt(running)
        factor[column, column] = pivot_value
        for target in range(column + 1, params):
            current = normal[target][column]
            for earlier in range(column):
                current = current - factor[target, earlier] * factor[column, earlier]
            factor[target, column] = current / pivot_value
    forward = []
    for target in range(params):
        current = moments[target]
        for earlier in range(target):
            current = current - factor[target, earlier] * forward[earlier]
        forward.append(current / factor[target, target])
    backward = [None] * params
    for target in reversed(range(params)):
        current = forward[target]
        for later in range(target + 1, params):
            current = current - factor[later, target] * backward[later]
        backward[target] = current / factor[target, target]
    return backward


def thirds(values):
    high = values.astype(jnp.bfloat16).astype(jnp.float32)
    rest = values - high
    middle = rest.astype(jnp.bfloat16).astype(jnp.float32)
    return [high, middle, rest - middle]


def stacked(values, rows):
    terms = thirds(values)
    spare = rows - 3 * values.shape[0]
    if spare:
        terms.append(jnp.zeros((spare, values.shape[1]), jnp.float32))
    return jnp.concatenate(terms, axis=0).astype(jnp.bfloat16)


def kernel(
    sizes,
    source_hbm, slot_hbm, owner_hbm, counts_hbm, partials_hbm, residual_hbm, weight_hbm, prior_hbm,
    updates_ref, fresh_ref, norm_ref,
    source_ref, slot_ref, owner_ref, counts_ref, partials_ref, residual_ref, weight_ref, prior_ref,
    out_buf, in_buf, hot_buf, back_out, back_in,
    load_sem, send_sem, recv_sem, back_send_sem, back_recv_sem,
):
    n, members, width, pad_slots = sizes
    params = partials_ref.shape[0]
    words = params + 2
    half = members // 2
    side = n // 2
    groups = n // members
    row_pairs = (
        (owner_hbm, owner_ref), (weight_hbm, weight_ref), (partials_hbm, partials_ref),
        (residual_hbm, residual_ref), (source_hbm, source_ref), (slot_hbm, slot_ref),
        (counts_hbm, counts_ref), (prior_hbm, prior_ref),
    )
    loads = [pltpu.make_async_copy(a, b, load_sem.at[i]) for i, (a, b) in enumerate(row_pairs)]
    for load in loads:
        load.start()
    src_local = counts_ref.shape[1]
    my_group, my_member = lax.axis_index("grp"), lax.axis_index("dev")
    me = my_group * members + my_member

    def target(i, far):
        group = (my_group + i // half) % groups
        member = (my_member // half + far) % 2 * half + (my_member % half + i % half) % half
        return group * members + member

    def origin(i, far):
        group = (my_group + groups - i // half) % groups
        member = (my_member // half + far) % 2 * half + (my_member % half + half - i % half) % half
        return group * members + member

    def coords(device):
        return (device // members, device % members)

    barrier = pltpu.get_barrier_semaphore()

    def greet(step, carry):
        peer = (me + step) % n
        pl.semaphore_signal(barrier, inc=1, device_id=coords(peer), device_id_type=MESH)
        return carry

    lax.fori_loop(1, n, greet, 0)

    loads[0].wait()
    position = me * src_local + lax.broadcasted_iota(jnp.int32, (src_local, LANES), 0)

    def invert(tile, total):
        ids = tile * LANES + lax.broadcasted_iota(jnp.int32, (1, LANES), 1)
        return total + jnp.where(owner_ref[pl.ds(tile, 1), :] == position, ids, 0)

    found = lax.fori_loop(0, owner_ref.shape[0], invert, jnp.zeros((src_local, LANES), jnp.int32))
    source_at = jnp.sum(found.astype(jnp.float32), axis=1, keepdims=True)
    for load in loads[1:]:
        load.wait()
    counts = counts_ref[...].astype(jnp.float32)
    diagonal = lax.broadcasted_iota(jnp.int32, (src_local, src_local), 0) == lax.broadcasted_iota(
        jnp.int32, (src_local, src_local), 1
    )
    count_column = jnp.sum(jnp.where(diagonal, counts, 0.0), axis=1, keepdims=True)
    first_cell = source_at * pad_slots
    end_cell = first_cell + count_column

    def prepare(step, carry):
        for part in range(UNROLL):
            k = step * UNROLL + part
            cols = pl.ds(pl.multiple_of(k * width, LANES), width)
            root = jnp.sqrt(weight_ref[:, cols])
            out_buf[k, 0:params, :] = partials_ref[:, cols] * root
            out_buf[k, params : params + 1, :] = residual_ref[:, cols] * root
            cell = source_ref[:, cols] * pad_slots + slot_ref[:, cols]
            out_buf[k, params + 1 : words, :] = cell.astype(jnp.float32)
            in_buf[k, words:SUBLANES, :] = jnp.zeros((SUBLANES - words, width), jnp.float32)
        return carry

    lax.fori_loop(0, n // UNROLL, prepare, 0)

    pl.semaphore_wait(barrier, n - 1)

    def forward(peer, slot):
        return pltpu.make_async_remote_copy(
            src_ref=out_buf.at[peer, pl.ds(0, words)],
            dst_ref=in_buf.at[slot, pl.ds(0, words)],
            send_sem=send_sem,
            recv_sem=recv_sem.at[slot],
            device_id=coords(peer),
            device_id_type=MESH,
        )

    forward(target(0, 1), me).start()

    def send(step, carry):
        forward(target(step, 1), me).start()
        forward(target(step, 0), me).start()
        return carry

    lax.fori_loop(1, side, send, 0)

    def absorb(k):
        rows = in_buf[k, 0:words, :]
        cell = rows[params + 1 : params + 2, :]
        hit = jnp.logical_and(cell >= first_cell, cell < end_cell)
        hot = jnp.where(hit, 1.0, 0.0).astype(jnp.bfloat16)
        hot_buf[k] = hot
        products = []
        for i in range(params):
            products.append(rows[i : i + 1, :] * in_buf[k])
        return lax.dot_general(
            stacked(jnp.concatenate(products, axis=0), LANES), hot, (((1,), (1,)), ((), ())),
            preferred_element_type=jnp.float32,
        )

    in_buf[me, 0:words, :] = out_buf[me, 0:words, :]
    far = origin(0, 1)
    forward(far, far).wait_recv()
    total = absorb(me) + absorb(far)

    def arrive(step, total):
        near, far = origin(step, 0), origin(step, 1)
        forward(near, near).wait_recv()
        forward(far, far).wait_recv()
        return total + absorb(near) + absorb(far)

    total = lax.fori_loop(1, side, arrive, total)

    height = params * SUBLANES
    sums = total[0:height] + total[height : 2 * height] + total[2 * height : 3 * height]
    normal = [[None] * params for _ in range(params)]
    for i in range(params):
        for j in range(i, params):
            entry = sums[i * SUBLANES + j : i * SUBLANES + j + 1]
            if i == j:
                entry = entry + prior_ref[i : i + 1, :]
            normal[i][j] = entry
            normal[j][i] = entry
    moments = [sums[i * SUBLANES + params : i * SUBLANES + params + 1] for i in range(params)]
    updates = solve_rows(normal, moments)
    for i in range(params):
        updates_ref[i : i + 1, :] = updates[i]
    blank = jnp.zeros((1, src_local), jnp.float32)
    table = jnp.concatenate(updates + [blank - 1.0] + [blank] * (SUBLANES - params - 1), axis=0)
    table = stacked(table, 4 * SUBLANES)

    def refit(step, squares):
        for part in range(UNROLL):
            k = step * UNROLL + part
            spread = jnp.dot(table, hot_buf[k], preferred_element_type=jnp.float32)
            spread = spread[0:SUBLANES] + spread[SUBLANES : 2 * SUBLANES] + spread[2 * SUBLANES : 3 * SUBLANES]
            fresh = -jnp.sum(in_buf[k] * spread, axis=0, keepdims=True)
            back_out[k, :, 0:width] = fresh
            squares = squares + fresh * fresh
        return squares

    squares = lax.fori_loop(0, n // UNROLL, refit, jnp.zeros((1, width), jnp.float32))
    lane = lax.broadcasted_iota(jnp.int32, (1, LANES), 1)
    square_sum = jnp.sum(squares, axis=1, keepdims=True)
    count_sum = jnp.sum(counts, axis=1, keepdims=True)
    tail = jnp.where(lane == 0, square_sum, jnp.where(lane == 1, count_sum, 0.0))

    def finish(k, carry):
        back_out[k, :, width : width + LANES] = tail
        return carry

    lax.fori_loop(0, n, finish, 0)
    back_in[me] = back_out[me]

    def backward(peer, slot):
        return pltpu.make_async_remote_copy(
            src_ref=back_out.at[peer],
            dst_ref=back_in.at[slot],
            send_sem=back_send_sem,
            recv_sem=back_recv_sem.at[slot],
            device_id=coords(peer),
            device_id_type=MESH,
        )

    backward(target(0, 1), me).start()

    def send_back(step, carry):
        backward(target(step, 1), me).start()
        backward(target(step, 0), me).start()
        return carry

    lax.fori_loop(1, side, send_back, 0)

    def collect(step, carry):
        peer = (me + n - step) % n
        backward(peer, peer).wait_recv()
        return carry

    lax.fori_loop(1, n, collect, 0)

    def gather_tails(k, tails):
        return tails + back_in[k, :, width : width + LANES]

    tails = lax.fori_loop(0, n, gather_tails, jnp.zeros((1, LANES), jnp.float32))
    square_total = jnp.sum(jnp.where(lane == 0, tails, 0.0), axis=1, keepdims=True)
    count_total = jnp.sum(jnp.where(lane == 1, tails, 0.0), axis=1, keepdims=True)
    norm = jnp.sqrt(square_total / count_total + 1e-06)
    norm_ref[...] = jnp.broadcast_to(norm, norm_ref.shape)
    scale = 1.0 / norm

    def emit(step, carry):
        for part in range(UNROLL):
            k = step * UNROLL + part
            cols = pl.ds(pl.multiple_of(k * width, LANES), width)
            fresh_ref[:, cols] = back_in[k, :, 0:width] * scale
        return carry

    lax.fori_loop(0, n // UNROLL, emit, 0)

    sent = (out_buf.at[pl.ds(0, n - 1), pl.ds(0, words)], back_out.at[pl.ds(0, n - 1)])
    for ref, semaphore in zip(sent, (send_sem, back_send_sem)):
        pltpu.make_async_remote_copy(
            src_ref=ref,
            dst_ref=ref,
            send_sem=semaphore,
            recv_sem=recv_sem.at[me],
            device_id=coords((me + 1) % n),
            device_id_type=MESH,
        ).wait_send()


def body(source_id, slot, owner, counts, partials, residual, weight, prior):
    members = lax.axis_size("dev")
    n = lax.axis_size("grp") * members
    params = partials.shape[0]
    row_count = residual.shape[0]
    src_local = counts.shape[0]
    block_rows = row_count // n
    width = -(-block_rows // LANES) * LANES

    def lay(array, fill):
        array = array.reshape(-1, row_count)
        if width == block_rows:
            return array
        blocks = array.reshape(-1, n, block_rows)
        blocks = jnp.pad(blocks, ((0, 0), (0, 0), (0, width - block_rows)), constant_values=fill)
        return blocks.reshape(-1, n * width)

    vmem = pl.BlockSpec(memory_space=pltpu.VMEM)
    operands = (
        lay(source_id, -1),
        lay(slot, 0),
        owner.reshape(-1, LANES),
        counts.reshape(1, src_local),
        lay(partials, 0),
        lay(residual, 0),
        lay(weight, 1),
        prior,
    )
    updates, standardized, norm = pl.pallas_call(
        functools.partial(kernel, (n, members, width, row_count // src_local)),
        out_shape=(
            jax.ShapeDtypeStruct((params, src_local), jnp.float32),
            jax.ShapeDtypeStruct((1, n * width), jnp.float32),
            jax.ShapeDtypeStruct((1, LANES), jnp.float32),
        ),
        in_specs=[pl.BlockSpec(memory_space=pltpu.HBM)] * len(operands),
        out_specs=(vmem, vmem, vmem),
        scratch_shapes=[pltpu.VMEM(operand.shape, operand.dtype) for operand in operands] + [
            pltpu.VMEM((n, SUBLANES, width), jnp.float32),
            pltpu.VMEM((n, SUBLANES, width), jnp.float32),
            pltpu.VMEM((n, src_local, width), jnp.bfloat16),
            pltpu.VMEM((n, 1, width + LANES), jnp.float32),
            pltpu.VMEM((n, 1, width + LANES), jnp.float32),
            pltpu.SemaphoreType.DMA((len(operands),)),
            pltpu.SemaphoreType.DMA,
            pltpu.SemaphoreType.DMA((n,)),
            pltpu.SemaphoreType.DMA,
            pltpu.SemaphoreType.DMA((n,)),
        ],
        compiler_params=pltpu.CompilerParams(
            collective_id=0, has_side_effects=True, vmem_limit_bytes=65000 * 1024
        ),
        name="exchange_fit",
    )(*operands)
    standardized = standardized.reshape(n, width)[:, :block_rows] if width != block_rows else standardized
    return (updates, standardized.reshape(row_count), norm[0, 0])


def solution(mesh):
    in_specs = (
        P(("grp", "dev")),
        P(("grp", "dev")),
        P(),
        P(("grp", "dev")),
        P(None, ("grp", "dev")),
        P(("grp", "dev")),
        P(("grp", "dev")),
        P(None, ("grp", "dev")),
    )
    out_specs = (P(None, ("grp", "dev")), P(("grp", "dev")), P())
    return jax.shard_map(body, mesh=mesh, in_specs=in_specs, out_specs=out_specs, check_vma=False)
```

```python
import functools

import jax
import jax.numpy as jnp
from jax import lax
from jax.experimental import pallas as pl
from jax.experimental.pallas import tpu as pltpu
from jax.sharding import PartitionSpec as P

LANES = 128
SUBLANES = 8
UNROLL = 4
MESH = pl.DeviceIdType.MESH


def solve_rows(normal, moments):
    params = len(moments)
    factor = {}
    inverse = []
    for column in range(params):
        running = normal[column][column]
        for earlier in range(column):
            running = running - factor[column, earlier] ** 2
        inverse.append(1.0 / jnp.sqrt(running))
        for target in range(column + 1, params):
            current = normal[target][column]
            for earlier in range(column):
                current = current - factor[target, earlier] * factor[column, earlier]
            factor[target, column] = current * inverse[column]
    forward = []
    for target in range(params):
        current = moments[target]
        for earlier in range(target):
            current = current - factor[target, earlier] * forward[earlier]
        forward.append(current * inverse[target])
    backward = [None] * params
    for target in reversed(range(params)):
        current = forward[target]
        for later in range(target + 1, params):
            current = current - factor[later, target] * backward[later]
        backward[target] = current * inverse[target]
    return backward


def thirds(values):
    high = values.astype(jnp.bfloat16).astype(jnp.float32)
    rest = values - high
    middle = rest.astype(jnp.bfloat16).astype(jnp.float32)
    return [high, middle, rest - middle]


def stacked(values, rows):
    terms = thirds(values)
    spare = rows - 3 * values.shape[0]
    if spare:
        terms.append(jnp.zeros((spare, values.shape[1]), jnp.float32))
    return jnp.concatenate(terms, axis=0).astype(jnp.bfloat16)


def kernel(
    sizes,
    source_hbm, slot_hbm, owner_hbm, counts_hbm, partials_hbm, residual_hbm, weight_hbm, prior_hbm,
    updates_ref, fresh_ref, norm_ref,
    source_ref, slot_ref, owner_ref, counts_ref, partials_ref, residual_ref, weight_ref, prior_ref,
    out_buf, in_buf, hot_buf, back_out, back_in, tail_out, tail_in,
    load_sem, tail_send_sem, tail_recv_sem, send_sem, recv_sem, back_send_sem, back_recv_sem,
):
    n, members, width, pad_slots = sizes
    params = partials_ref.shape[0]
    words = params + 2
    half = members // 2
    side = n // 2
    groups = n // members
    row_pairs = (
        (owner_hbm, owner_ref), (weight_hbm, weight_ref), (partials_hbm, partials_ref),
        (residual_hbm, residual_ref), (source_hbm, source_ref), (slot_hbm, slot_ref),
        (counts_hbm, counts_ref), (prior_hbm, prior_ref),
    )
    loads = [pltpu.make_async_copy(a, b, load_sem.at[i]) for i, (a, b) in enumerate(row_pairs)]
    for load in loads:
        load.start()
    src_local = counts_ref.shape[1]
    my_group, my_member = lax.axis_index("grp"), lax.axis_index("dev")
    me = my_group * members + my_member

    def target(i, far):
        group = (my_group + i // half) % groups
        member = (my_member // half + far) % 2 * half + (my_member % half + i % half) % half
        return group * members + member

    def origin(i, far):
        group = (my_group + groups - i // half) % groups
        member = (my_member // half + far) % 2 * half + (my_member % half + half - i % half) % half
        return group * members + member

    def coords(device):
        return (device // members, device % members)

    barrier = pltpu.get_barrier_semaphore()

    def greet(step, carry):
        peer = (me + step) % n
        pl.semaphore_signal(barrier, inc=1, device_id=coords(peer), device_id_type=MESH)
        return carry

    lax.fori_loop(1, n, greet, 0)

    for load in loads:
        load.wait()
    def prepare(step, carry):
        for part in range(UNROLL):
            k = step * UNROLL + part
            cols = pl.ds(pl.multiple_of(k * width, LANES), width)
            root = jnp.sqrt(weight_ref[:, cols])
            out_buf[k, 0:params, :] = partials_ref[:, cols] * root
            out_buf[k, params : params + 1, :] = residual_ref[:, cols] * root
            cell = source_ref[:, cols] * pad_slots + slot_ref[:, cols]
            out_buf[k, params + 1 : words, :] = cell.astype(jnp.float32)
            in_buf[k, words:SUBLANES, :] = jnp.zeros((SUBLANES - words, width), jnp.float32)
        return carry

    lax.fori_loop(0, n // UNROLL, prepare, 0)

    pl.semaphore_wait(barrier, n - 1)

    def forward(peer, slot):
        return pltpu.make_async_remote_copy(
            src_ref=out_buf.at[peer, pl.ds(0, words)],
            dst_ref=in_buf.at[slot, pl.ds(0, words)],
            send_sem=send_sem,
            recv_sem=recv_sem.at[slot],
            device_id=coords(peer),
            device_id_type=MESH,
        )

    forward(target(0, 1), me).start()

    def send(step, carry):
        forward(target(step, 1), me).start()
        forward(target(step, 0), me).start()
        return carry

    lax.fori_loop(1, side, send, 0)

    position = me * src_local + lax.broadcasted_iota(jnp.int32, (src_local, LANES), 0)

    def invert(tile, total):
        ids = tile * LANES + lax.broadcasted_iota(jnp.int32, (1, LANES), 1)
        return total + jnp.where(owner_ref[pl.ds(tile, 1), :] == position, ids, 0)

    found = lax.fori_loop(0, owner_ref.shape[0], invert, jnp.zeros((src_local, LANES), jnp.int32))
    source_at = jnp.sum(found.astype(jnp.float32), axis=1, keepdims=True)
    counts = counts_ref[...].astype(jnp.float32)
    diagonal = lax.broadcasted_iota(jnp.int32, (src_local, src_local), 0) == lax.broadcasted_iota(
        jnp.int32, (src_local, src_local), 1
    )
    count_column = jnp.sum(jnp.where(diagonal, counts, 0.0), axis=1, keepdims=True)
    first_cell = source_at * pad_slots
    end_cell = first_cell + count_column

    def absorb(k):
        rows = in_buf[k, 0:words, :]
        cell = rows[params + 1 : params + 2, :]
        hit = jnp.logical_and(cell >= first_cell, cell < end_cell)
        hot = jnp.where(hit, 1.0, 0.0).astype(jnp.bfloat16)
        hot_buf[k] = hot
        products = []
        for i in range(params):
            products.append(rows[i : i + 1, :] * in_buf[k])
        return lax.dot_general(
            stacked(jnp.concatenate(products, axis=0), LANES), hot, (((1,), (1,)), ((), ())),
            preferred_element_type=jnp.float32,
        )

    in_buf[me, 0:words, :] = out_buf[me, 0:words, :]
    far = origin(0, 1)
    forward(far, far).wait_recv()
    total = absorb(me) + absorb(far)

    def arrive(step, total):
        near, far = origin(step, 0), origin(step, 1)
        forward(near, near).wait_recv()
        forward(far, far).wait_recv()
        return total + absorb(near) + absorb(far)

    total = lax.fori_loop(1, side, arrive, total)

    height = params * SUBLANES
    sums = total[0:height] + total[height : 2 * height] + total[2 * height : 3 * height]
    normal = [[None] * params for _ in range(params)]
    for i in range(params):
        for j in range(i, params):
            entry = sums[i * SUBLANES + j : i * SUBLANES + j + 1]
            if i == j:
                entry = entry + prior_ref[i : i + 1, :]
            normal[i][j] = entry
            normal[j][i] = entry
    moments = [sums[i * SUBLANES + params : i * SUBLANES + params + 1] for i in range(params)]
    updates = solve_rows(normal, moments)
    for i in range(params):
        updates_ref[i : i + 1, :] = updates[i]
    blank = jnp.zeros((1, src_local), jnp.float32)
    table = jnp.concatenate(updates + [blank - 1.0] + [blank] * (SUBLANES - params - 1), axis=0)
    table = stacked(table, 4 * SUBLANES)

    def backward(peer, slot):
        return pltpu.make_async_remote_copy(
            src_ref=back_out.at[peer],
            dst_ref=back_in.at[slot],
            send_sem=back_send_sem,
            recv_sem=back_recv_sem.at[slot],
            device_id=coords(peer),
            device_id_type=MESH,
        )

    def summary(peer, slot):
        return pltpu.make_async_remote_copy(
            src_ref=tail_out,
            dst_ref=tail_in.at[slot],
            send_sem=tail_send_sem,
            recv_sem=tail_recv_sem.at[slot],
            device_id=coords(peer),
            device_id_type=MESH,
        )

    def refit(k):
        spread = jnp.dot(table, hot_buf[k], preferred_element_type=jnp.float32)
        spread = spread[0:SUBLANES] + spread[SUBLANES : 2 * SUBLANES] + spread[2 * SUBLANES : 3 * SUBLANES]
        fresh = -jnp.sum(in_buf[k] * spread, axis=0, keepdims=True)
        back_out[k] = fresh
        return fresh * fresh

    def refit_far(step, squares):
        for part in range(UNROLL):
            squares = squares + refit(target(step * UNROLL + part, 1))
        for part in range(UNROLL):
            peer = target(step * UNROLL + part, 1)
            backward(peer, me).start()
        return squares

    def refit_near(step, squares):
        for part in range(UNROLL):
            squares = squares + refit(target(step * UNROLL + part, 0))
        return squares

    squares = lax.fori_loop(0, side // UNROLL, refit_far, jnp.zeros((1, width), jnp.float32))
    squares = lax.fori_loop(0, side // UNROLL, refit_near, squares)
    lane = lax.broadcasted_iota(jnp.int32, (1, LANES), 1)
    square_sum = jnp.sum(squares, axis=1, keepdims=True)
    count_sum = jnp.sum(counts, axis=1, keepdims=True)
    tail_out[...] = jnp.where(lane == 0, square_sum, jnp.where(lane == 1, count_sum, 0.0))

    def send_far_tail(step, carry):
        summary(target(step, 1), me).start()
        return carry

    def send_near(step, carry):
        backward(target(step, 0), me).start()
        summary(target(step, 0), me).start()
        return carry

    lax.fori_loop(0, side, send_far_tail, 0)
    lax.fori_loop(1, side, send_near, 0)
    back_in[me] = back_out[me]
    tail_in[me] = tail_out[...]

    def collect(step, carry):
        peer = (me + n - step) % n
        backward(peer, peer).wait_recv()
        summary(peer, peer).wait_recv()
        return carry

    lax.fori_loop(1, n, collect, 0)

    def gather_tails(k, tails):
        return tails + tail_in[k]

    tails = lax.fori_loop(0, n, gather_tails, jnp.zeros((1, LANES), jnp.float32))
    square_total = jnp.sum(jnp.where(lane == 0, tails, 0.0), axis=1, keepdims=True)
    count_total = jnp.sum(jnp.where(lane == 1, tails, 0.0), axis=1, keepdims=True)
    norm = jnp.sqrt(square_total / count_total + 1e-06)
    norm_ref[...] = jnp.broadcast_to(norm, norm_ref.shape)
    scale = 1.0 / norm

    def emit(step, carry):
        for part in range(UNROLL):
            k = step * UNROLL + part
            cols = pl.ds(pl.multiple_of(k * width, LANES), width)
            fresh_ref[:, cols] = back_in[k] * scale
        return carry

    lax.fori_loop(0, n // UNROLL, emit, 0)

    sent = (out_buf.at[pl.ds(0, n - 1), pl.ds(0, words)], back_out.at[pl.ds(0, n - 1)], tail_in.at[pl.ds(0, n - 1)])
    for ref, semaphore in zip(sent, (send_sem, back_send_sem, tail_send_sem)):
        pltpu.make_async_remote_copy(
            src_ref=ref,
            dst_ref=ref,
            send_sem=semaphore,
            recv_sem=recv_sem.at[me],
            device_id=coords((me + 1) % n),
            device_id_type=MESH,
        ).wait_send()


def release(a_ref, b_ref, c_ref, a_out, b_out, c_out, sem):
    pairs = ((a_ref, a_out), (b_ref, b_out), (c_ref, c_out))
    copies = [pltpu.make_async_copy(x, y, sem.at[i]) for i, (x, y) in enumerate(pairs)]
    for copy in copies:
        copy.start()
    for copy in copies:
        copy.wait()


def body(source_id, slot, owner, counts, partials, residual, weight, prior):
    members = lax.axis_size("dev")
    n = lax.axis_size("grp") * members
    params = partials.shape[0]
    row_count = residual.shape[0]
    src_local = counts.shape[0]
    block_rows = row_count // n
    width = -(-block_rows // LANES) * LANES

    def lay(array, fill):
        array = array.reshape(-1, row_count)
        if width == block_rows:
            return array
        blocks = array.reshape(-1, n, block_rows)
        blocks = jnp.pad(blocks, ((0, 0), (0, 0), (0, width - block_rows)), constant_values=fill)
        return blocks.reshape(-1, n * width)

    vmem = pl.BlockSpec(memory_space=pltpu.VMEM)
    operands = (
        lay(source_id, -1),
        lay(slot, 0),
        owner.reshape(-1, LANES),
        counts.reshape(1, src_local),
        lay(partials, 0),
        lay(residual, 0),
        lay(weight, 1),
        prior,
    )
    updates, standardized, norm = pl.pallas_call(
        functools.partial(kernel, (n, members, width, row_count // src_local)),
        out_shape=(
            jax.ShapeDtypeStruct((params, src_local), jnp.float32),
            jax.ShapeDtypeStruct((1, n * width), jnp.float32),
            jax.ShapeDtypeStruct((1, LANES), jnp.float32),
        ),
        in_specs=[pl.BlockSpec(memory_space=pltpu.HBM)] * len(operands),
        out_specs=(vmem, vmem, vmem),
        scratch_shapes=[pltpu.VMEM(operand.shape, operand.dtype) for operand in operands] + [
            pltpu.VMEM((n, SUBLANES, width), jnp.float32),
            pltpu.VMEM((n, SUBLANES, width), jnp.float32),
            pltpu.VMEM((n, src_local, width), jnp.bfloat16),
            pltpu.VMEM((n, 1, width), jnp.float32),
            pltpu.VMEM((n, 1, width), jnp.float32),
            pltpu.VMEM((1, LANES), jnp.float32),
            pltpu.VMEM((n, 1, LANES), jnp.float32),
            pltpu.SemaphoreType.DMA((len(operands),)),
            pltpu.SemaphoreType.DMA,
            pltpu.SemaphoreType.DMA((n,)),
            pltpu.SemaphoreType.DMA,
            pltpu.SemaphoreType.DMA((n,)),
            pltpu.SemaphoreType.DMA,
            pltpu.SemaphoreType.DMA((n,)),
        ],
        compiler_params=pltpu.CompilerParams(
            collective_id=0, has_side_effects=True, vmem_limit_bytes=65000 * 1024
        ),
        name="exchange_fit",
    )(*operands)
    results = (updates, standardized, norm)
    updates, standardized, norm = pl.pallas_call(
        release,
        out_shape=tuple(jax.ShapeDtypeStruct(r.shape, r.dtype) for r in results),
        in_specs=[vmem] * 3,
        out_specs=[pl.BlockSpec(memory_space=pltpu.HBM)] * 3,
        scratch_shapes=[pltpu.SemaphoreType.DMA((3,))],
        name="release",
    )(*results)
    standardized = standardized.reshape(n, width)[:, :block_rows] if width != block_rows else standardized
    return (updates, standardized.reshape(row_count), norm[0, 0])


def solution(mesh):
    in_specs = (
        P(("grp", "dev")),
        P(("grp", "dev")),
        P(),
        P(("grp", "dev")),
        P(None, ("grp", "dev")),
        P(("grp", "dev")),
        P(("grp", "dev")),
        P(None, ("grp", "dev")),
    )
    out_specs = (P(None, ("grp", "dev")), P(("grp", "dev")), P())
    return jax.shard_map(body, mesh=mesh, in_specs=in_specs, out_specs=out_specs, check_vma=False)
```

```python
import functools

import jax
import jax.numpy as jnp
from jax import lax
from jax.experimental import pallas as pl
from jax.experimental.pallas import tpu as pltpu
from jax.sharding import PartitionSpec as P

LANES = 128
SUBLANES = 8
UNROLL = 4
MESH = pl.DeviceIdType.MESH


def solve_rows(normal, moments):
    params = len(moments)
    factor = {}
    inverse = []
    for column in range(params):
        running = normal[column][column]
        for earlier in range(column):
            running = running - factor[column, earlier] ** 2
        inverse.append(1.0 / jnp.sqrt(running))
        for target in range(column + 1, params):
            current = normal[target][column]
            for earlier in range(column):
                current = current - factor[target, earlier] * factor[column, earlier]
            factor[target, column] = current * inverse[column]
    forward = []
    for target in range(params):
        current = moments[target]
        for earlier in range(target):
            current = current - factor[target, earlier] * forward[earlier]
        forward.append(current * inverse[target])
    backward = [None] * params
    for target in reversed(range(params)):
        current = forward[target]
        for later in range(target + 1, params):
            current = current - factor[later, target] * backward[later]
        backward[target] = current * inverse[target]
    return backward


def thirds(values):
    high = values.astype(jnp.bfloat16).astype(jnp.float32)
    rest = values - high
    middle = rest.astype(jnp.bfloat16).astype(jnp.float32)
    return [high, middle, rest - middle]


def stacked(values, rows):
    terms = thirds(values)
    spare = rows - 3 * values.shape[0]
    if spare:
        terms.append(jnp.zeros((spare, values.shape[1]), jnp.float32))
    return jnp.concatenate(terms, axis=0).astype(jnp.bfloat16)


def kernel(
    sizes,
    source_hbm, slot_hbm, owner_hbm, counts_hbm, partials_hbm, residual_hbm, weight_hbm, prior_hbm,
    updates_ref, fresh_ref, norm_ref,
    source_ref, slot_ref, owner_ref, counts_ref, partials_ref, residual_ref, weight_ref, prior_ref,
    out_buf, in_buf, hot_buf, back_out, back_in, tail_out, tail_in,
    load_sem, tail_send_sem, tail_recv_sem, send_sem, recv_sem, back_send_sem, back_recv_sem,
):
    n, members, width, pad_slots = sizes
    params = partials_ref.shape[0]
    words = params + 2
    half = members // 2
    side = n // 2
    groups = n // members
    row_pairs = (
        (owner_hbm, owner_ref), (weight_hbm, weight_ref), (partials_hbm, partials_ref),
        (residual_hbm, residual_ref), (source_hbm, source_ref), (slot_hbm, slot_ref),
        (counts_hbm, counts_ref), (prior_hbm, prior_ref),
    )
    loads = [pltpu.make_async_copy(a, b, load_sem.at[i]) for i, (a, b) in enumerate(row_pairs)]
    for load in loads:
        load.start()
    src_local = counts_ref.shape[1]
    my_group, my_member = lax.axis_index("grp"), lax.axis_index("dev")
    me = my_group * members + my_member

    def target(i, far):
        group = (my_group + i // half) % groups
        member = (my_member // half + far) % 2 * half + (my_member % half + i % half) % half
        return group * members + member

    def origin(i, far):
        group = (my_group + groups - i // half) % groups
        member = (my_member // half + far) % 2 * half + (my_member % half + half - i % half) % half
        return group * members + member

    def coords(device):
        return (device // members, device % members)

    barrier = pltpu.get_barrier_semaphore()

    def greet(step, carry):
        peer = (me + step) % n
        pl.semaphore_signal(barrier, inc=1, device_id=coords(peer), device_id_type=MESH)
        return carry

    lax.fori_loop(1, n, greet, 0)

    for load in loads:
        load.wait()
    def prepare(step, carry):
        for part in range(UNROLL):
            k = step * UNROLL + part
            cols = pl.ds(pl.multiple_of(k * width, LANES), width)
            root = jnp.sqrt(weight_ref[:, cols])
            out_buf[k, 0:params, :] = partials_ref[:, cols] * root
            out_buf[k, params : params + 1, :] = residual_ref[:, cols] * root
            cell = source_ref[:, cols] * pad_slots + slot_ref[:, cols]
            out_buf[k, params + 1 : words, :] = cell.astype(jnp.float32)
            in_buf[k, words:SUBLANES, :] = jnp.zeros((SUBLANES - words, width), jnp.float32)
        return carry

    lax.fori_loop(0, n // UNROLL, prepare, 0)

    pl.semaphore_wait(barrier, n - 1)

    def forward(peer, slot):
        return pltpu.make_async_remote_copy(
            src_ref=out_buf.at[peer, pl.ds(0, words)],
            dst_ref=in_buf.at[slot, pl.ds(0, words)],
            send_sem=send_sem,
            recv_sem=recv_sem.at[slot],
            device_id=coords(peer),
            device_id_type=MESH,
        )

    forward(target(0, 1), me).start()

    def send(step, carry):
        forward(target(step, 1), me).start()
        forward(target(step, 0), me).start()
        return carry

    lax.fori_loop(1, side, send, 0)

    position = me * src_local + lax.broadcasted_iota(jnp.int32, (src_local, LANES), 0)

    def invert(tile, total):
        ids = tile * LANES + lax.broadcasted_iota(jnp.int32, (1, LANES), 1)
        return total + jnp.where(owner_ref[pl.ds(tile, 1), :] == position, ids, 0)

    found = lax.fori_loop(0, owner_ref.shape[0], invert, jnp.zeros((src_local, LANES), jnp.int32))
    source_at = jnp.sum(found.astype(jnp.float32), axis=1, keepdims=True)
    counts = counts_ref[...].astype(jnp.float32)
    diagonal = lax.broadcasted_iota(jnp.int32, (src_local, src_local), 0) == lax.broadcasted_iota(
        jnp.int32, (src_local, src_local), 1
    )
    count_column = jnp.sum(jnp.where(diagonal, counts, 0.0), axis=1, keepdims=True)
    first_cell = source_at * pad_slots
    end_cell = first_cell + count_column

    def absorb(k):
        rows = in_buf[k, 0:words, :]
        cell = rows[params + 1 : params + 2, :]
        hit = jnp.logical_and(cell >= first_cell, cell < end_cell)
        hot = jnp.where(hit, 1.0, 0.0).astype(jnp.bfloat16)
        hot_buf[k] = hot
        products = []
        for i in range(params):
            products.append(rows[i : i + 1, :] * in_buf[k])
        return lax.dot_general(
            stacked(jnp.concatenate(products, axis=0), LANES), hot, (((1,), (1,)), ((), ())),
            preferred_element_type=jnp.float32,
        )

    in_buf[me, 0:words, :] = out_buf[me, 0:words, :]
    far = origin(0, 1)
    forward(far, far).wait_recv()
    total = absorb(me) + absorb(far)

    def arrive(step, total):
        near, far = origin(step, 0), origin(step, 1)
        forward(near, near).wait_recv()
        forward(far, far).wait_recv()
        return total + absorb(near) + absorb(far)

    total = lax.fori_loop(1, side, arrive, total)

    height = params * SUBLANES
    sums = total[0:height] + total[height : 2 * height] + total[2 * height : 3 * height]
    normal = [[None] * params for _ in range(params)]
    for i in range(params):
        for j in range(i, params):
            entry = sums[i * SUBLANES + j : i * SUBLANES + j + 1]
            if i == j:
                entry = entry + prior_ref[i : i + 1, :]
            normal[i][j] = entry
            normal[j][i] = entry
    moments = [sums[i * SUBLANES + params : i * SUBLANES + params + 1] for i in range(params)]
    updates = solve_rows(normal, moments)
    for i in range(params):
        updates_ref[i : i + 1, :] = updates[i]
    blank = jnp.zeros((1, src_local), jnp.float32)
    table = jnp.concatenate(updates + [blank - 1.0] + [blank] * (SUBLANES - params - 1), axis=0)
    table = stacked(table, 4 * SUBLANES)

    def backward(peer, slot):
        return pltpu.make_async_remote_copy(
            src_ref=back_out.at[peer],
            dst_ref=back_in.at[slot],
            send_sem=back_send_sem,
            recv_sem=back_recv_sem,
            device_id=coords(peer),
            device_id_type=MESH,
        )

    def summary(peer, slot):
        return pltpu.make_async_remote_copy(
            src_ref=tail_out,
            dst_ref=tail_in.at[slot],
            send_sem=tail_send_sem,
            recv_sem=tail_recv_sem,
            device_id=coords(peer),
            device_id_type=MESH,
        )

    def refit(k):
        spread = jnp.dot(table, hot_buf[k], preferred_element_type=jnp.float32)
        spread = spread[0:SUBLANES] + spread[SUBLANES : 2 * SUBLANES] + spread[2 * SUBLANES : 3 * SUBLANES]
        fresh = -jnp.sum(in_buf[k] * spread, axis=0, keepdims=True)
        back_out[k, :, 0:width] = fresh
        return fresh * fresh

    def refit_far(step, squares):
        for part in range(UNROLL):
            squares = squares + refit(target(step * UNROLL + part, 1))
        return squares

    def refit_near(step, squares):
        for part in range(UNROLL):
            squares = squares + refit(target(step * UNROLL + part, 0))
        return squares

    squares = lax.fori_loop(0, side // UNROLL, refit_far, jnp.zeros((1, width), jnp.float32))
    squares = lax.fori_loop(0, side // UNROLL, refit_near, squares)
    lane = lax.broadcasted_iota(jnp.int32, (1, LANES), 1)
    square_sum = jnp.sum(squares, axis=1, keepdims=True)
    count_sum = jnp.sum(counts, axis=1, keepdims=True)
    tail_out[...] = jnp.where(lane == 0, square_sum, jnp.where(lane == 1, count_sum, 0.0))

    def finish(step, carry):
        for part in range(UNROLL):
            back_out[step * UNROLL + part, :, width : width + LANES] = tail_out[...]
        return carry

    lax.fori_loop(0, n // UNROLL, finish, 0)

    def send_far_tail(step, carry):
        backward(target(step, 1), me).start()
        return carry

    def send_near(step, carry):
        backward(target(step, 0), me).start()
        return carry

    lax.fori_loop(0, side, send_far_tail, 0)
    lax.fori_loop(1, side, send_near, 0)
    back_in[me] = back_out[me]

    others = pl.ds(0, n - 1)
    for ref, semaphore in ((back_in.at[others], back_recv_sem),):
        pltpu.make_async_remote_copy(
            src_ref=ref,
            dst_ref=ref,
            send_sem=back_send_sem,
            recv_sem=semaphore,
            device_id=coords((me + 1) % n),
            device_id_type=MESH,
        ).wait_recv()

    def gather_tails(k, tails):
        return tails + back_in[k, :, width : width + LANES]

    tails = lax.fori_loop(0, n, gather_tails, jnp.zeros((1, LANES), jnp.float32))
    square_total = jnp.sum(jnp.where(lane == 0, tails, 0.0), axis=1, keepdims=True)
    count_total = jnp.sum(jnp.where(lane == 1, tails, 0.0), axis=1, keepdims=True)
    norm = jnp.sqrt(square_total / count_total + 1e-06)
    norm_ref[...] = jnp.broadcast_to(norm, norm_ref.shape)
    scale = 1.0 / norm

    def emit(step, carry):
        for part in range(UNROLL):
            k = step * UNROLL + part
            cols = pl.ds(pl.multiple_of(k * width, LANES), width)
            fresh_ref[:, cols] = back_in[k, :, 0:width] * scale
        return carry

    lax.fori_loop(0, n // UNROLL, emit, 0)

    sent = (out_buf.at[pl.ds(0, n - 1), pl.ds(0, words)], back_out.at[pl.ds(0, n - 1)])
    for ref, semaphore in zip(sent, (send_sem, back_send_sem)):
        pltpu.make_async_remote_copy(
            src_ref=ref,
            dst_ref=ref,
            send_sem=semaphore,
            recv_sem=recv_sem.at[me],
            device_id=coords((me + 1) % n),
            device_id_type=MESH,
        ).wait_send()


def release(a_ref, b_ref, c_ref, a_out, b_out, c_out, sem):
    pairs = ((a_ref, a_out), (b_ref, b_out), (c_ref, c_out))
    copies = [pltpu.make_async_copy(x, y, sem.at[i]) for i, (x, y) in enumerate(pairs)]
    for copy in copies:
        copy.start()
    for copy in copies:
        copy.wait()


def body(source_id, slot, owner, counts, partials, residual, weight, prior):
    members = lax.axis_size("dev")
    n = lax.axis_size("grp") * members
    params = partials.shape[0]
    row_count = residual.shape[0]
    src_local = counts.shape[0]
    block_rows = row_count // n
    width = -(-block_rows // LANES) * LANES

    def lay(array, fill):
        array = array.reshape(-1, row_count)
        if width == block_rows:
            return array
        blocks = array.reshape(-1, n, block_rows)
        blocks = jnp.pad(blocks, ((0, 0), (0, 0), (0, width - block_rows)), constant_values=fill)
        return blocks.reshape(-1, n * width)

    vmem = pl.BlockSpec(memory_space=pltpu.VMEM)
    operands = (
        lay(source_id, -1),
        lay(slot, 0),
        owner.reshape(-1, LANES),
        counts.reshape(1, src_local),
        lay(partials, 0),
        lay(residual, 0),
        lay(weight, 1),
        prior,
    )
    updates, standardized, norm = pl.pallas_call(
        functools.partial(kernel, (n, members, width, row_count // src_local)),
        out_shape=(
            jax.ShapeDtypeStruct((params, src_local), jnp.float32),
            jax.ShapeDtypeStruct((1, n * width), jnp.float32),
            jax.ShapeDtypeStruct((1, LANES), jnp.float32),
        ),
        in_specs=[pl.BlockSpec(memory_space=pltpu.HBM)] * len(operands),
        out_specs=(vmem, vmem, vmem),
        scratch_shapes=[pltpu.VMEM(operand.shape, operand.dtype) for operand in operands] + [
            pltpu.VMEM((n, SUBLANES, width), jnp.float32),
            pltpu.VMEM((n, SUBLANES, width), jnp.float32),
            pltpu.VMEM((n, src_local, width), jnp.bfloat16),
            pltpu.VMEM((n, 1, width + LANES), jnp.float32),
            pltpu.VMEM((n, 1, width + LANES), jnp.float32),
            pltpu.VMEM((1, LANES), jnp.float32),
            pltpu.VMEM((n, 1, LANES), jnp.float32),
            pltpu.SemaphoreType.DMA((len(operands),)),
            pltpu.SemaphoreType.DMA,
            pltpu.SemaphoreType.DMA,
            pltpu.SemaphoreType.DMA,
            pltpu.SemaphoreType.DMA((n,)),
            pltpu.SemaphoreType.DMA,
            pltpu.SemaphoreType.DMA,
        ],
        compiler_params=pltpu.CompilerParams(
            collective_id=0, has_side_effects=True, vmem_limit_bytes=65000 * 1024
        ),
        name="exchange_fit",
    )(*operands)
    results = (updates, standardized, norm)
    updates, standardized, norm = pl.pallas_call(
        release,
        out_shape=tuple(jax.ShapeDtypeStruct(r.shape, r.dtype) for r in results),
        in_specs=[vmem] * 3,
        out_specs=[pl.BlockSpec(memory_space=pltpu.HBM)] * 3,
        scratch_shapes=[pltpu.SemaphoreType.DMA((3,))],
        name="release",
    )(*results)
    standardized = standardized.reshape(n, width)[:, :block_rows] if width != block_rows else standardized
    return (updates, standardized.reshape(row_count), norm[0, 0])


def solution(mesh):
    in_specs = (
        P(("grp", "dev")),
        P(("grp", "dev")),
        P(),
        P(("grp", "dev")),
        P(None, ("grp", "dev")),
        P(("grp", "dev")),
        P(("grp", "dev")),
        P(None, ("grp", "dev")),
    )
    out_specs = (P(None, ("grp", "dev")), P(("grp", "dev")), P())
    return jax.shard_map(body, mesh=mesh, in_specs=in_specs, out_specs=out_specs, check_vma=False)
```
